256 devices in a mesh: fsdp: 64 (over z, y_lo, x), tp: 4 (over y_hi, core).
Axes of the slice: x: 4, y: 4 (y_hi: 2, y_lo: 2; y = y_hi * 2 + y_lo), z: 8, core: 2. Of those that a mesh axis runs over, the one named last changes fastest.
Arguments:
- tokens: bfloat16 [1024, 4096], P('fsdp', 'tp'), may hold values from -6 to 6
- route_logits: bfloat16 [1024, 2], P('fsdp'), may hold values from -6 to 6
- route_ids: int32 [1024, 2], P('fsdp'), may hold values from 0 to 7, all different within a row; in each aligned block of 1024 rows (0 to 1023, 1024 to 2047, ...) at most 512 rows name the same one
- gate_codes: bfloat16 [8, 14336, 4096], P(None, 'fsdp', 'tp'), may hold values from -4 to 4
- gate_scales: float32 [8, 14336, 32], P(None, 'fsdp', 'tp'), may hold values from 0.008 to 0.03
- up_codes: bfloat16 [8, 14336, 4096], P(None, 'fsdp', 'tp'), may hold values from -4 to 4
- up_scales: float32 [8, 14336, 32], P(None, 'fsdp', 'tp'), may hold values from 0.008 to 0.03
- down_codes: bfloat16 [8, 14336, 4096], P(None, 'fsdp', 'tp'), may hold values from -4 to 4
- down_scales: float32 [8, 14336, 32], P(None, 'fsdp', 'tp'), may hold values from 0.004 to 0.016
Outputs:
- mixed: bfloat16 [1024, 4096], P('fsdp', 'tp')
The draws below stay inside these ranges and needn't reach their ends.
Inputs may be any that keep to these rules, and one draw needn't show every extreme that they name: `route_ids`: each row names two different experts; over all 1024 rows no expert is named more than 512 times, a bound that some block reaches.
All inputs are finite; a program needn't handle non-finite values.
Results may differ from the reference program's by a relative error of at most 0.011.
Values may be sent and summed in bfloat16 or wider, within the bound.
A program may use at most 128 MiB of HBM per device.

```python
import math
import jax
import jax.numpy as jnp
import numpy as np
from jax import lax

D = 4096
FF = 14336
EXPERTS = 8
TOP = 2
QBLOCK = 128
TOKENS = 1024
CAP = 512


def level_of(rng, extent, shards, low, largest):
    level, own = 1.0, jax.random.fold_in(rng, 6)
    for position, parts in shards:
        draws = jnp.exp(jax.random.uniform(jax.random.fold_in(own, position), (parts,), jnp.float32, low / len(shards), largest / len(shards)))
        level = level * jnp.repeat(draws, extent[position] // parts).reshape([-1 if axis == position else 1 for axis in range(len(extent))])
    return level


def assign_block(own_key, own, number, rows, amount, top, bound, lean):
    sequence = jax.random.permutation(own_key, amount)
    heavy_load, usual = load_shares(amount, rows * top, bound, lean, True), load_shares(amount, rows * top, bound, lean, False)
    places = jnp.arange(amount)

    def named(tallies, turn):
        used = int((tallies > 0).sum())
        fixed = max(1, used // 4)
        shifted = fixed + (places - fixed + turn * (used - fixed)) % max(1, amount - fixed)
        return jnp.zeros((amount,), jnp.int32).at[sequence[jnp.where(places < fixed, places, shifted)]].set(jnp.asarray(tallies, jnp.int32))

    tallies = jnp.where(number % 4 == 0, named(heavy_load, number // 4), named(usual, number - number // 4 - 1))
    mixed = jax.random.permutation(jax.random.fold_in(own, 3), amount)
    donor, sink = mixed[0:amount // 2 * 2:2], mixed[1:amount // 2 * 2:2]
    room = jnp.minimum(tallies[donor] - 1, bound - tallies[sink]) // 2
    room = jnp.where((donor == sequence[0]) | (sink == sequence[0]) | (tallies[sink] == 0), 0, jnp.maximum(room, 0))
    shifted = jax.random.randint(jax.random.fold_in(own, 4), (amount // 2,), 0, 1 << 20) % (room + 1)
    tallies = tallies.at[donor].add(-shifted).at[sink].add(shifted)
    labels = jnp.searchsorted(jnp.cumsum(tallies), jnp.arange(rows * top), side="right").astype(jnp.int32)
    grid = labels.reshape(top, rows).T
    grid = grid[jax.random.permutation(jax.random.fold_in(own, 1), rows)]
    turn = jax.random.randint(jax.random.fold_in(own, 2), (rows, 1), 0, top)
    return jnp.take_along_axis(grid, (jnp.arange(top)[None, :] + turn) % top, axis=1)


def load_shares(number_of, total, limit, skew, full):
    portions = [(1 << 20) // math.isqrt(rank ** skew) + 1 for rank in range(1, number_of + 1)]
    largest = limit if full else min(limit, max(-(-total // number_of), total * portions[0] // sum(portions)))
    least = 1 if total - largest >= number_of - 1 else 0
    given, rest = [largest] + [least] * (number_of - 1), total - largest - least * (number_of - 1)
    while rest > 0:
        free = [i for i in range(1, number_of) if given[i] < largest] or [i for i in range(1, number_of) if given[i] < limit]
        pool, budget = sum([portions[i] for i in free]), rest
        for i in free:
            more = min(limit - given[i], max(1, budget * portions[i] // pool), rest)
            given[i] = given[i] + more
            rest = rest - more
    return np.array(given)


def centred(stream_key, dims, spread, bound, shards=(), kind=jnp.bfloat16):
    array = spread * jax.random.normal(stream_key, dims, jnp.float32)
    if shards:
        array = array * level_of(stream_key, dims, shards, -0.22, 0.18)
    return jnp.clip(array, -bound, bound).astype(kind)


def setup_inputs(seed: int = 0) -> dict:
    streams_of = jax.random.split(jax.random.key(seed), 10)
    tokens = centred(streams_of[0], (TOKENS, D), 1.0, 6.0, ((0, 64), (1, 4)))
    route_logits = centred(streams_of[1], (TOKENS, TOP), 1.5, 6.0, ((0, 64),))
    route_ids_keys = jax.random.split(jax.random.fold_in(streams_of[2], 1), TOKENS // TOKENS)
    route_ids_turns = jax.random.permutation(jax.random.fold_in(streams_of[2], 3), TOKENS // TOKENS)
    route_ids = jax.vmap(lambda own, number: assign_block(jax.random.fold_in(streams_of[2], 2), own, number, TOKENS, EXPERTS, TOP, CAP, 2))(route_ids_keys, route_ids_turns).reshape((TOKENS, TOP))
    gate_codes = centred(streams_of[3], (EXPERTS, FF, D), 1.0, 4.0, ((1, 64), (2, 4)))
    gate_scales = jnp.clip(jnp.exp(math.log(0.03) - 1.3217558 * jax.random.uniform(streams_of[4], (EXPERTS, FF, D // QBLOCK), jnp.float32) ** level_of(streams_of[4], (EXPERTS, FF, D // QBLOCK), ((1, 64), (2, 4)), -0.2, 0.2)), 0.008, 0.03)
    up_codes = centred(streams_of[5], (EXPERTS, FF, D), 1.0, 4.0, ((1, 64), (2, 4)))
    up_scales = jnp.clip(jnp.exp(math.log(0.03) - 1.3217558 * jax.random.uniform(streams_of[6], (EXPERTS, FF, D // QBLOCK), jnp.float32) ** level_of(streams_of[6], (EXPERTS, FF, D // QBLOCK), ((1, 64), (2, 4)), -0.2, 0.2)), 0.008, 0.03)
    down_codes = centred(streams_of[7], (EXPERTS, FF, D), 1.0, 4.0, ((1, 64), (2, 4)))
    down_scales = jnp.clip(jnp.exp(math.log(0.016) - 1.3862944 * jax.random.uniform(streams_of[8], (EXPERTS, FF, D // QBLOCK), jnp.float32) ** level_of(streams_of[8], (EXPERTS, FF, D // QBLOCK), ((1, 64), (2, 4)), -0.2, 0.2)), 0.004, 0.016)
    return dict(tokens=tokens, route_logits=route_logits, route_ids=route_ids, gate_codes=gate_codes, gate_scales=gate_scales, up_codes=up_codes, up_scales=up_scales, down_codes=down_codes, down_scales=down_scales)


def dispatch(route_ids, experts, capacity):
    flat_ids = route_ids.reshape(-1).astype(jnp.int32)
    one_hot = (flat_ids[:, None] == jnp.arange(experts, dtype=jnp.int32)[None, :]).astype(jnp.int32)
    earlier = (jnp.cumsum(one_hot, axis=0) - one_hot).astype(jnp.int32)
    slot_rank = jnp.sum(earlier * one_hot, axis=1).astype(jnp.int32)
    return (flat_ids * capacity + slot_rank).astype(jnp.int32)


def expand_cols(codes, scales):
    leading, row_count, col_count = codes.shape
    blocks = scales.shape[2]
    grouped = codes.astype(jnp.float32).reshape(leading, row_count, blocks, col_count // blocks)
    grouped = grouped * scales[:, :, :, None]
    return grouped.reshape(leading, row_count, col_count).astype(jnp.bfloat16)


def reference(tokens, route_logits, route_ids, gate_codes, gate_scales, up_codes, up_scales, down_codes, down_scales):
    places = dispatch(route_ids, EXPERTS, CAP)
    repeated = jnp.repeat(tokens, 2, axis=0)
    slots = jnp.zeros((EXPERTS * CAP, D), jnp.bfloat16).at[places].set(repeated).reshape(EXPERTS, CAP, D)

    def one_expert(pieces):
        rows_in, gate_code, gate_scale, up_code, up_scale, down_code, down_scale = pieces
        gate_w = expand_cols(gate_code[None], gate_scale[None])[0]
        up_w = expand_cols(up_code[None], up_scale[None])[0]
        down_w = expand_cols(down_code[None], down_scale[None])[0]
        contract = (((1,), (1,)), ((), ()))
        gate_sum = lax.dot_general(rows_in, gate_w, contract, preferred_element_type=jnp.float32)
        up_sum = lax.dot_general(rows_in, up_w, contract, preferred_element_type=jnp.float32)
        hidden = (jax.nn.silu(gate_sum) * up_sum).astype(jnp.bfloat16)
        return jnp.dot(hidden, down_w, preferred_element_type=jnp.float32)

    outputs = lax.map(one_expert, (slots, gate_codes, gate_scales, up_codes, up_scales, down_codes, down_scales))
    routed = outputs.reshape(EXPERTS * CAP, D)[places].reshape(TOKENS, 2, D)
    logits = route_logits.astype(jnp.float32)
    first_w = jax.nn.sigmoid(logits[:, 0] - logits[:, 1])
    second_w = jax.nn.sigmoid(logits[:, 1] - logits[:, 0])
    mixed = routed[:, 0] * first_w[:, None] + routed[:, 1] * second_w[:, None]
    return mixed.astype(jnp.bfloat16)
```

```python
import jax
import jax.numpy as jnp
from jax import lax
from jax.experimental import pallas as pl
from jax.experimental.pallas import tpu as pltpu
from jax.sharding import PartitionSpec as P

F32, BF16 = jnp.float32, jnp.bfloat16
MESH = pl.DeviceIdType.MESH
E, FH, DK = 8, 224, 1024
XW = DK + 128
HW = DK // 2
OFFSETS = (0, 1, -1, 2, -2, 3, -3, 4)


def pos_of(r):
    return OFFSETS.index(r)


def kernel(
    tok_ref, log_ref, ids_ref, gc_ref, gs_ref, uc_ref, us_ref, dc_ref, ds_ref,
    out_ref,
    wgu, dw, sg, su, sd, xbuf, xt, acc, rt, pb, rb, yb, yr, hb, am, part, r1, s2, r2, zs, rz,
    w_sem, s_sem, p_send, p_recv, g_send, g_recv, t_send, t_recv, x_send, x_recv, z_send, z_recv,
):
    f, t = lax.axis_index("fsdp"), lax.axis_index("tp")
    z, blk = f // 8, f % 8
    y, x = blk // 4, blk % 4
    yh, core = t // 2, t % 2
    xa = x + 1 - 2 * (x % 2)
    xb = 3 - x
    xd = 3 - xa

    def fid(zz, yy, xx):
        return (zz * 2 + yy) * 4 + xx

    def dev(ff, tt):
        return {"fsdp": ff, "tp": tt}

    def zoff(r):
        return (z + r + 8) % 8

    sibling = dev(f, yh * 2 + 1 - core)
    partner = dev(f, (1 - yh) * 2 + core)
    sends = []

    def copy(src, dst, ssem, rsem, to):
        return pltpu.make_async_remote_copy(
            src_ref=src, dst_ref=dst, send_sem=ssem, recv_sem=rsem, device_id=to, device_id_type=MESH
        )

    def send(src, dst, ssem, rsem, to):
        c = copy(src, dst, ssem, rsem, to)
        c.start()
        sends.append(c)

    def arrived(dst, ssem, rsem):
        copy(dst, dst, ssem, rsem, sibling).wait_recv()

    def w_copy(kind, e):
        src = (gc_ref, uc_ref, dc_ref)[kind]
        dst = (wgu.at[e, pl.ds(0, FH)], wgu.at[e, pl.ds(FH, FH)], dw.at[e, pl.ds(0, FH)])[kind]
        return pltpu.make_async_copy(src.at[e], dst, w_sem.at[kind, e])

    def s_copy(kind):
        src, dst = ((gs_ref, sg), (us_ref, su), (ds_ref, sd))[kind]
        return pltpu.make_async_copy(src, dst, s_sem.at[kind])

    s_copy(0).start()
    s_copy(1).start()
    for kind in (0, 1, 2):
        if kind == 2:
            s_copy(2).start()

        @pl.loop(0, E)
        def _(e):
            w_copy(kind, e).start()

    lane = lax.broadcasted_iota(jnp.int32, (16, 128), 1)
    ids = ids_ref[...].astype(F32)
    logits = log_ref[...].astype(F32)
    extra = jnp.where(
        lane == 0,
        ids[:, 0:1],
        jnp.where(lane == 1, ids[:, 1:2], jnp.where(lane == 2, logits[:, 0:1], jnp.where(lane == 3, logits[:, 1:2], 0.0))),
    )
    xbuf[0, blk, :, 0:DK] = tok_ref[...]
    xbuf[0, blk, :, DK:XW] = extra.astype(BF16)

    barrier = pltpu.get_barrier_semaphore()
    friends = [dev(z * 8 + (blk + d) % 8, t) for d in range(1, 8)]
    friends += [dev(fid(zoff(r), yy, x), t) for r in OFFSETS[1:] for yy in (y, 1 - y)]
    friends += [sibling, partner]
    for to in friends:
        pl.semaphore_signal(barrier, inc=1, device_id=to, device_id_type=MESH)
    pl.semaphore_wait(barrier, len(friends))

    for d in range(1, 8):
        send(xbuf.at[0, blk], xbuf.at[0, blk], p_send.at[d], p_recv.at[d], dev(z * 8 + (blk + d) % 8, t))

    def plane_arrived():
        for d in range(1, 8):
            arrived(xbuf.at[0, (blk + 8 - d) % 8], p_send.at[d], p_recv.at[d])

    def ring_piece(way, s, p):
        return (p_of(way, s), pl.ds(4 * p, 4))

    def p_of(way, s):
        if s == 0:
            return 0
        return pos_of(4) if s == 4 else pos_of(-s if way == 0 else s)

    def ring(s, p):
        for way in (0, 1):
            if s > 1:
                at, rows = ring_piece(way, s - 1, p)
                arrived(xbuf.at[at, rows], g_send.at[way, s - 1, p], g_recv.at[way, s - 1, p])
            if s < 4 or p == way:
                a, rows = ring_piece(way, s - 1, p)
                b, _ = ring_piece(way, s, p)
                to = dev(fid(zoff(1 if way == 0 else -1), y, x), t)
                send(xbuf.at[a, rows], xbuf.at[b, rows], g_send.at[way, s, p], g_recv.at[way, s, p], to)

    def ring_end():
        for way in (0, 1):
            at, rows = ring_piece(way, 4, way)
            arrived(xbuf.at[at, rows], g_send.at[way, 4, way], g_recv.at[way, 4, way])

    def scale_gate_up(lo, hi):
        @pl.loop(lo, hi)
        def _(e):
            w_copy(0, e).wait()
            w_copy(1, e).wait()
            for at, sc in ((0, sg), (FH, su)):
                for b in range(8):
                    cols = slice(b * 128, (b + 1) * 128)
                    w = wgu[e, at : at + FH, cols].astype(F32) * sc[e, :, b : b + 1]
                    wgu[e, at : at + FH, cols] = w.astype(BF16)

    def scale_down(lo, hi):
        @pl.loop(lo, hi)
        def _(e):
            w_copy(2, e).wait()
            dw[e, FH:256, :] = jnp.zeros((256 - FH, DK), BF16)
            for b in range(8):
                cols = slice(b * 128, (b + 1) * 128)
                w = dw[e, 0:FH, cols].astype(F32) * sd[e, :, b : b + 1]
                dw[e, 0:FH, cols] = w.astype(BF16)

    def gate_up(c):
        rows = xbuf[2 * c : 2 * c + 2].reshape(256, XW)
        xt[...] = rows[:, 0:DK].T
        route = rows[:, DK:XW].astype(F32).T
        for hh in (0, 1):
            rt[c, hh] = route[0:8, hh * 128 : (hh + 1) * 128]
        picks = [[route[k : k + 1, hh * 128 : (hh + 1) * 128] for hh in (0, 1)] for k in (0, 1)]

        def one(e):
            o = jnp.dot(wgu[e], xt[...], preferred_element_type=F32)
            for k in (0, 1):
                for hh in (0, 1):
                    mine = o[:, hh * 128 : (hh + 1) * 128]
                    hit = picks[k][hh] == jnp.asarray(e, jnp.int32).astype(F32)
                    acc[c, k, hh] = jnp.where(hit, mine, 0.0 if isinstance(e, int) else acc[c, k, hh])

        one(0)
        pl.loop(1, E)(one)
        pb[c] = acc[c, 1 - core].astype(BF16)
        send(pb.at[c], rb.at[c], t_send.at[0, c], t_recv.at[0, c], sibling)

    def pair_sum(c, hh):
        return acc[c, core, hh] + rb[c, hh].astype(F32)

    def core_sum(c):
        arrived(rb.at[c], t_send.at[0, c], t_recv.at[0, c])
        yb[c] = pair_sum(c, 1 - yh).astype(BF16)
        send(yb.at[c], yr.at[c], t_send.at[1, c], t_recv.at[1, c], partner)

    def activate(c):
        arrived(yr.at[c], t_send.at[1, c], t_recv.at[1, c])
        total = pair_sum(c, yh) + yr[c].astype(F32)
        gate, up = total[0:FH], total[FH : 2 * FH]
        route = rt[c, yh]
        diff = route[3:4] - route[2:3]
        w = 1.0 / (1.0 + jnp.exp(jnp.where(core == 0, diff, -diff)))
        hb[c, core, yh] = (gate / (1.0 + jnp.exp(-gate)) * up * w).astype(BF16)
        mine = hb.at[c, core, yh]
        send(mine, mine, t_send.at[2, c], t_recv.at[2, c], partner)
        send(mine, mine, t_send.at[3, c], t_recv.at[3, c], sibling)

    def pass_on(c):
        theirs = hb.at[c, core, 1 - yh]
        arrived(theirs, t_send.at[2, c], t_recv.at[2, c])
        send(theirs, theirs, t_send.at[4, c], t_recv.at[4, c], sibling)

    def down(c):
        arrived(hb.at[c, 1 - core, yh], t_send.at[3, c], t_recv.at[3, c])
        arrived(hb.at[c, 1 - core, 1 - yh], t_send.at[4, c], t_recv.at[4, c])
        pad = jnp.zeros((256 - FH, 128), F32)
        for hh in (0, 1):
            here = slice(hh * 128, (hh + 1) * 128)
            route = xbuf[2 * c + hh, :, :, DK:XW].reshape(128, 128).astype(F32)
            units = [jnp.concatenate([hb[c, k, hh].astype(F32), pad], axis=0).T for k in (0, 1)]
            for e in range(E):
                both = jnp.where(route[:, 0:1] == float(e), units[0], 0.0)
                both = jnp.where(route[:, 1:2] == float(e), units[1], both)
                am[here, e * 256 : (e + 1) * 256] = both.astype(BF16)
        for j in range(4):
            w = dw[:, :, j * 256 : (j + 1) * 256].reshape(E * 256, 256)
            o = jnp.dot(am[...], w, preferred_element_type=F32)
            half, at = j // 2, (j % 2) * 256
            part[half, 2 * c : 2 * c + 2, :, :, :, at : at + 256] = o.astype(BF16).reshape(2, 2, 4, 16, 256)
        two = pl.ds(2 * c, 2)
        for half, first in ((0, xa), (1, xb)):
            for j, at in ((0, first), (1, xd)):
                send(
                    part.at[half, two, :, at], r1.at[half, two, :, j],
                    x_send.at[c, half, j], x_recv.at[c, half, j], dev(fid(z, y, first), t),
                )

    def x_first(c):
        two = pl.ds(2 * c, 2)
        for half, second in ((0, xb), (1, xa)):
            for j in (0, 1):
                arrived(r1.at[half, two, :, j], x_send.at[c, half, j], x_recv.at[c, half, j])
            s2[half, two] = (part[half, two, :, second].astype(F32) + r1[half, two, :, 1].astype(F32)).astype(BF16)
            send(
                s2.at[half, two], r2.at[half, two],
                x_send.at[c, half, 2], x_recv.at[c, half, 2], dev(fid(z, y, second), t),
            )

    def x_second(c):
        two = pl.ds(2 * c, 2)
        for half in (0, 1):
            arrived(r2.at[half, two], x_send.at[c, half, 2], x_recv.at[c, half, 2])
            total = part[half, two, :, x].astype(F32) + r1[half, two, :, 0].astype(F32) + r2[half, two].astype(F32)
            zs[two, :, half] = total.astype(BF16)
        for at in (2 * c, 2 * c + 1):
            for dy in (0, 1):
                if at or dy:
                    yy = (y + dy) % 2
                    to = dev(fid(zoff(OFFSETS[at]), yy, x), t)
                    send(zs.at[at, yy], rz.at[at, dy], z_send.at[at, dy], z_recv.at[at, dy], to)

    def finish():
        total = zs[0, y].astype(F32)
        for at in range(8):
            for dy in (0, 1):
                if at or dy:
                    arrived(rz.at[at, dy], z_send.at[at, dy], z_recv.at[at, dy])
                    total = total + rz[at, dy].astype(F32)
        for half in (0, 1):
            out_ref[:, half * HW : (half + 1) * HW] = total[half].astype(BF16)

    s_copy(0).wait()
    s_copy(1).wait()
    scale_gate_up(0, 2)
    plane_arrived()
    ring(1, 0), ring(1, 1)
    scale_gate_up(2, 8)
    ring(2, 0), ring(2, 1)
    gate_up(0)
    ring(3, 0)
    s_copy(2).wait()
    scale_down(0, 4)
    core_sum(0)
    ring(3, 1)
    gate_up(1)
    ring(4, 0)
    scale_down(4, 8)
    activate(0), core_sum(1)
    ring(4, 1)
    pass_on(0)
    gate_up(2)
    down(0)
    activate(1), core_sum(2)
    ring_end()
    gate_up(3)
    pass_on(1)
    x_first(0)
    down(1)
    core_sum(3), activate(2)
    x_second(0)
    x_first(1)
    pass_on(2)
    down(2)
    activate(3)
    x_second(1)
    pass_on(3)
    x_first(2)
    down(3)
    x_second(2)
    x_first(3)
    x_second(3)
    finish()
    for c in sends:
        c.wait_send()


def body(tokens, logits, ids, gate_codes, gate_scales, up_codes, up_scales, down_codes, down_scales):
    vmem = pl.BlockSpec(memory_space=pltpu.VMEM)
    hbm = pl.BlockSpec(memory_space=pl.ANY)
    sems = pltpu.SemaphoreType.DMA
    return pl.pallas_call(
        kernel,
        out_shape=jax.ShapeDtypeStruct((16, DK), BF16),
        in_specs=[vmem] * 3 + [hbm] * 6,
        out_specs=vmem,
        scratch_shapes=[
            pltpu.VMEM((E, 2 * FH, DK), BF16),
            pltpu.VMEM((E, 256, DK), BF16),
            pltpu.VMEM((E, FH, 8), F32),
            pltpu.VMEM((E, FH, 8), F32),
            pltpu.VMEM((E, FH, 8), F32),
            pltpu.VMEM((8, 8, 16, XW), BF16),
            pltpu.VMEM((DK, 256), BF16),
            pltpu.VMEM((4, 2, 2, 2 * FH, 128), F32),
            pltpu.VMEM((4, 2, 8, 128), F32),
            pltpu.VMEM((4, 2, 2 * FH, 128), BF16),
            pltpu.VMEM((4, 2, 2 * FH, 128), BF16),
            pltpu.VMEM((4, 2 * FH, 128), BF16),
            pltpu.VMEM((4, 2 * FH, 128), BF16),
            pltpu.VMEM((4, 2, 2, FH, 128), BF16),
            pltpu.VMEM((256, E * 256), BF16),
            pltpu.VMEM((2, 8, 2, 4, 16, HW), BF16),
            pltpu.VMEM((2, 8, 2, 2, 16, HW), BF16),
            pltpu.VMEM((2, 8, 2, 16, HW), BF16),
            pltpu.VMEM((2, 8, 2, 16, HW), BF16),
            pltpu.VMEM((8, 2, 2, 16, HW), BF16),
            pltpu.VMEM((8, 2, 2, 16, HW), BF16),
            sems((3, E)),
            sems((3,)),
            sems((8,)),
            sems((8,)),
            sems((2, 5, 2)),
            sems((2, 5, 2)),
            sems((5, 4)),
            sems((5, 4)),
            sems((4, 2, 3)),
            sems((4, 2, 3)),
            sems((8, 2)),
            sems((8, 2)),
        ],
        compiler_params=pltpu.CompilerParams(
            collective_id=0, has_side_effects=True, vmem_limit_bytes=60 * 1024 * 1024
        ),
        name="expert_step",
    )(tokens, logits, ids, gate_codes, gate_scales, up_codes, up_scales, down_codes, down_scales)


def solution(mesh):
    wide = P(None, "fsdp", "tp")
    in_specs = (P("fsdp", "tp"), P("fsdp", None), P("fsdp", None)) + (wide,) * 6
    return jax.shard_map(body, mesh=mesh, in_specs=in_specs, out_specs=P("fsdp", "tp"), check_vma=False)
```

```python
import jax
import jax.numpy as jnp
from jax import lax
from jax.experimental import pallas as pl
from jax.experimental.pallas import tpu as pltpu
from jax.sharding import PartitionSpec as P

F32, BF16 = jnp.float32, jnp.bfloat16
MESH = pl.DeviceIdType.MESH
E, FH, DK = 8, 224, 1024
GROUP = 4
HW = DK // 2
OFFSETS = (1, -1, 3, -3, 4, 2, -2, 0)


def pos_of(r):
    return OFFSETS.index(r)


def kernel(
    tok_ref, log_ref, ids_ref, gc_ref, gs_ref, uc_ref, us_ref, dc_ref, ds_ref,
    out_ref,
    wgu, dw, sc, tgu, td, flip, xbuf, rbuf, xt, acc, rt, pb, rb, yb, yr, hb, am, part, r1, s2, r2, zs, rz,
    w_sem, out_sem, g_recv, h_recv, t_recv, x_recv, z_recv,
):
    f, t = lax.axis_index("fsdp"), lax.axis_index("tp")
    z, blk = f // 8, f % 8
    y, x = blk // 4, blk % 4
    yh, core = t // 2, t % 2
    xa = x + 1 - 2 * (x % 2)
    xb = 3 - x
    xd = 3 - xa
    left, right, far = (x + 3) % 4, (x + 1) % 4, (x + 2) % 4
    own = pos_of(0)

    def fid(zz, yy, xx):
        return (zz * 2 + yy) * 4 + xx

    def dev(ff, tt):
        return {"fsdp": ff, "tp": tt}

    def zoff(r):
        return (z + r + 8) % 8

    sibling = dev(f, yh * 2 + 1 - core)
    partner = dev(f, (1 - yh) * 2 + core)

    def copy(src, dst, ssem, rsem, to):
        return pltpu.make_async_remote_copy(
            src_ref=src, dst_ref=dst, send_sem=ssem, recv_sem=rsem, device_id=to, device_id_type=MESH
        )

    G, H, PB, YB, HB, X1, X2, Z = range(8)

    def send(src, dst, kind, rsem, to):
        copy(src, dst, out_sem.at[kind], rsem, to).start()

    def arrived(dst, rsem):
        copy(dst, dst, out_sem.at[G], rsem, sibling).wait_recv()

    def all_sent(src, kind):
        copy(src, src, out_sem.at[kind], out_sem.at[kind], sibling).wait_send()

    barrier = pltpu.get_barrier_semaphore()
    friends = [dev(fid(zoff(r), (y + dy) % 2, x), t) for r in OFFSETS for dy in (0, 1) if r or dy]
    friends += [dev(fid(z, y, left), t), dev(fid(z, y, right), t), sibling, partner]
    for to in friends:
        pl.semaphore_signal(barrier, inc=1, device_id=to, device_id_type=MESH)

    def w_copy(kind):
        src = (gc_ref, uc_ref, dc_ref)[kind]
        dst = (wgu.at[:, pl.ds(0, FH)], wgu.at[:, pl.ds(FH, FH)], dw.at[:, pl.ds(0, FH)])[kind]
        return pltpu.make_async_copy(src, dst, w_sem.at[kind])

    def s_copy(kind):
        return pltpu.make_async_copy((gs_ref, us_ref, ds_ref)[kind], sc.at[kind], w_sem.at[3 + kind])

    for kind in range(3):
        s_copy(kind).start()
    for kind in range(3):
        w_copy(kind).start()

    flip[...] = jnp.zeros((8, 128), F32)
    flip[0:2, 0:16] = ids_ref[...].astype(F32)
    flip[2:4, 0:16] = log_ref[...].astype(F32)
    xbuf[own, y, x] = tok_ref[...]
    rbuf[own, y, x] = jnp.sum(pltpu.roll(flip[...], 0, 1, stride=16, stride_axis=0), axis=0, keepdims=True)

    def enter():
        pl.semaphore_wait(barrier, len(friends))

    def both(src, dst, kind, at, to, routes=True):
        send(xbuf.at[src], xbuf.at[dst], G, g_recv.at[kind, at], to)
        if routes:
            send(rbuf.at[src[:3]], rbuf.at[dst[:3]], H, h_recv.at[kind, at], to)

    every = slice(None)
    low, high = slice(0, HW), slice(HW, DK)

    def spread():
        for at, r in enumerate(OFFSETS):
            for dy in (0, 1):
                if r or dy:
                    both((own, y, x), (at, y, x), 0, at, dev(fid(zoff(-r), (y + dy) % 2, x), t))

    def along_x(at):
        rows = every if OFFSETS[at] else 1 - y
        arrived(xbuf.at[at, rows, x], g_recv.at[0, at])
        arrived(rbuf.at[at, rows, x], h_recv.at[0, at])
        for to in (right, left):
            both((at, every, x), (at, every, x), 1, at, dev(fid(z, y, to), t))

    def along_x_again(at):
        arrived(xbuf.at[at, 0], g_recv.at[1, at])
        arrived(rbuf.at[at, 0], h_recv.at[1, at])
        here = (at, every, left, every, low)
        both(here, here, 2, at, dev(fid(z, y, right), t))
        here = (at, every, right, every, high)
        both(here, here, 2, at, dev(fid(z, y, left), t), False)

    def plane_complete(at):
        arrived(xbuf.at[at, every, far], g_recv.at[2, at])
        arrived(rbuf.at[at, every, far], h_recv.at[2, at])

    lanes = lax.broadcasted_iota(jnp.int32, (8, 128), 1) // 16
    on_row = lanes == lax.broadcasted_iota(jnp.int32, (8, 128), 0)

    def unpack_routes(at):
        rows = jnp.concatenate([rbuf[at, i // 4, i % 4] for i in range(8)], axis=0)
        rows = pltpu.roll(rows, 0, 1, stride=16, stride_axis=0)
        for v in range(4):
            turned = pltpu.roll(rows, 128 - 16 * v, 1) if v else rows
            rt[at // 2, at % 2, v : v + 1, :] = jnp.sum(jnp.where(on_row, turned, 0.0), axis=0, keepdims=True)

    def turn_scales():
        for kind in range(3):
            s_copy(kind).wait()
        for kinds, dst in ((slice(0, 2), tgu), (slice(2, 3), td)):
            rows = sc[kinds].reshape(-1, FH)
            if rows.shape[0] < 128:
                rows = jnp.concatenate([rows, jnp.zeros((128 - rows.shape[0], FH), F32)], axis=0)
            dst[0:128] = rows[:, 0:128].T
            dst[128:FH] = jnp.concatenate([rows[:, 128:FH], jnp.zeros((128, 256 - FH), F32)], axis=1).T[0 : FH - 128]
        for kind in range(3):
            w_copy(kind).wait()

    def scale_gate_up(lo, hi):
        @pl.loop(lo, hi)
        def _(e):
            scales = pltpu.roll(tgu[...], (128 - 8 * e) % 128, 1)
            for at, lane in ((0, 0), (FH, 64)):
                for b in range(8):
                    cols = slice(b * 128, (b + 1) * 128)
                    w = wgu[e, at : at + FH, cols].astype(F32) * scales[:, lane + b : lane + b + 1]
                    wgu[e, at : at + FH, cols] = w.astype(BF16)

    def scale_down(lo, hi):
        @pl.loop(lo, hi)
        def _(e):
            dw[e, FH:256, :] = jnp.zeros((256 - FH, DK), BF16)
            scales = pltpu.roll(td[...], (128 - 8 * e) % 128, 1)
            for b in range(8):
                cols = slice(b * 128, (b + 1) * 128)
                w = dw[e, 0:FH, cols].astype(F32) * scales[:, b : b + 1]
                dw[e, 0:FH, cols] = w.astype(BF16)

    def gate_up(c):
        for hh in (0, 1):
            plane_complete(2 * c + hh)
            unpack_routes(2 * c + hh)
        xt[...] = xbuf[2 * c : 2 * c + 2].reshape(256, DK).T
        picks = [[rt[c, hh, k : k + 1, :] for hh in (0, 1)] for k in (0, 1)]

        @pl.loop(0, E // GROUP)
        def _(g):
            w = wgu[pl.ds(g * GROUP, GROUP)].reshape(GROUP * 2 * FH, DK)
            o = jnp.dot(w, xt[...], preferred_element_type=F32)
            for i in range(GROUP):
                e = jnp.asarray(g * GROUP + i, jnp.int32).astype(F32)
                for k in (0, 1):
                    for hh in (0, 1):
                        mine = o[i * 2 * FH : (i + 1) * 2 * FH, hh * 128 : (hh + 1) * 128]
                        acc[c, k, hh] = jnp.where(picks[k][hh] == e, mine, acc[c, k, hh])

        pb[c] = acc[c, 1 - core].astype(BF16)
        send(pb.at[c], rb.at[c], PB, t_recv.at[0, c], sibling)

    def pair_sum(c, hh):
        return acc[c, core, hh] + rb[c, hh].astype(F32)

    def core_sum(c):
        arrived(rb.at[c], t_recv.at[0, c])
        yb[c] = pair_sum(c, 1 - yh).astype(BF16)
        send(yb.at[c], yr.at[c], YB, t_recv.at[1, c], partner)

    def activate(c):
        arrived(yr.at[c], t_recv.at[1, c])
        total = pair_sum(c, yh) + yr[c].astype(F32)
        gate, up = total[0:FH], total[FH : 2 * FH]
        route = rt[c, yh]
        diff = route[3:4] - route[2:3]
        w = 1.0 / (1.0 + jnp.exp(jnp.where(core == 0, diff, -diff)))
        hb[c, core, yh] = (gate / (1.0 + jnp.exp(-gate)) * up * w).astype(BF16)
        mine = hb.at[c, core, yh]
        send(mine, mine, HB, t_recv.at[2, c], partner)
        send(mine, mine, HB, t_recv.at[3, c], sibling)

    def pass_on(c):
        theirs = hb.at[c, core, 1 - yh]
        arrived(theirs, t_recv.at[2, c])
        send(theirs, theirs, HB, t_recv.at[3, c], sibling)

    def down(c):
        arrived(hb.at[c, 1 - core], t_recv.at[3, c])
        pad = jnp.zeros((256 - FH, 128), F32)
        for hh in (0, 1):
            here = slice(hh * 128, (hh + 1) * 128)
            route = rt[c, hh].T
            units = [jnp.concatenate([hb[c, k, hh].astype(F32), pad], axis=0).T for k in (0, 1)]
            for e in range(E):
                both = jnp.where(route[:, 0:1] == float(e), units[0], 0.0)
                both = jnp.where(route[:, 1:2] == float(e), units[1], both)
                am[here, e * 256 : (e + 1) * 256] = both.astype(BF16)
        for j in range(4):
            w = dw[:, :, j * 256 : (j + 1) * 256].reshape(E * 256, 256)
            o = jnp.dot(am[...], w, preferred_element_type=F32)
            half, at = j // 2, (j % 2) * 256
            part[half, 2 * c : 2 * c + 2, :, :, :, at : at + 256] = o.astype(BF16).reshape(2, 2, 4, 16, 256)
        two = pl.ds(2 * c, 2)
        for half, first in ((0, xa), (1, xb)):
            for j, at in ((1, xd), (0, first)):
                send(part.at[half, two, :, at], r1.at[half, two, :, j], X1, x_recv.at[j, c], dev(fid(z, y, first), t))

    def x_first(c):
        two = pl.ds(2 * c, 2)
        arrived(r1.at[:, two, :, 1], x_recv.at[1, c])
        for half, second in ((0, xb), (1, xa)):
            s2[half, two] = (part[half, two, :, second].astype(F32) + r1[half, two, :, 1].astype(F32)).astype(BF16)
            send(s2.at[half, two], r2.at[half, two], X2, x_recv.at[2, c], dev(fid(z, y, second), t))

    def x_second(c):
        two = pl.ds(2 * c, 2)
        arrived(r1.at[:, two, :, 0], x_recv.at[0, c])
        arrived(r2.at[:, two], x_recv.at[2, c])
        for half in (0, 1):
            total = part[half, two, :, x].astype(F32) + r1[half, two, :, 0].astype(F32) + r2[half, two].astype(F32)
            zs[two, :, half] = total.astype(BF16)
        for at in (2 * c, 2 * c + 1):
            for dy in (0, 1):
                if OFFSETS[at] or dy:
                    yy = (y + dy) % 2
                    to = dev(fid(zoff(OFFSETS[at]), yy, x), t)
                    send(zs.at[at, yy], rz.at[2 * at + dy], Z, z_recv, to)

    def finish():
        arrived(rz.at[pl.ds(0, 15)], z_recv)
        total = zs[own, y].astype(F32)
        for i in range(16):
            if i != 2 * own:
                total = total + rz[i].astype(F32)
        for half in (0, 1):
            out_ref[:, half * HW : (half + 1) * HW] = total[half].astype(BF16)

    def leave():
        all_sent(xbuf.reshape(64, 16, DK).at[pl.ds(0, 63)], G)
        all_sent(rbuf.reshape(64, 1, 128).at[pl.ds(0, 63)], H)
        all_sent(pb, PB)
        all_sent(yb, YB)
        all_sent(hb.at[pl.ds(0, 3)], HB)
        all_sent(r1, X1)
        all_sent(s2, X2)
        all_sent(rz.at[pl.ds(0, 15)], Z)

    schedule = (
        (enter,),
        (spread,),
        (turn_scales,),
        (scale_gate_up, 0, 6),
        (along_x, 0), (along_x, 1),
        (scale_gate_up, 6, 8),
        (along_x, 7),
        (scale_down, 0, 3),
        (along_x, 2), (along_x, 3),
        (along_x_again, 0), (along_x_again, 1),
        (along_x, 4),
        (scale_down, 3, 6),
        (along_x, 5), (along_x, 6),
        (along_x_again, 2), (along_x_again, 3),
        (gate_up, 0),
        (along_x_again, 4), (along_x_again, 7),
        (core_sum, 0),
        (along_x_again, 5), (along_x_again, 6),
        (gate_up, 1),
        (core_sum, 1),
        (scale_down, 6, 8),
        (gate_up, 2),
        (activate, 0), (core_sum, 2),
        (gate_up, 3),
        (pass_on, 0), (activate, 1),
        (core_sum, 3),
        (down, 0),
        (activate, 2), (pass_on, 1),
        (down, 1),
        (activate, 3), (pass_on, 2),
        (x_first, 0),
        (down, 2),
        (x_first, 1),
        (pass_on, 3),
        (x_second, 0),
        (down, 3),
        (x_first, 2),
        (x_second, 1),
        (x_first, 3),
        (x_second, 2),
        (x_second, 3),
        (finish,),
        (leave,),
    )
    for step, *args in schedule:
        with jax.named_scope("_".join([step.__name__, *map(str, args)])):
            step(*args)


def body(tokens, logits, ids, gate_codes, gate_scales, up_codes, up_scales, down_codes, down_scales):
    vmem = pl.BlockSpec(memory_space=pltpu.VMEM)
    hbm = pl.BlockSpec(memory_space=pl.ANY)
    sems = pltpu.SemaphoreType.DMA
    return pl.pallas_call(
        kernel,
        out_shape=jax.ShapeDtypeStruct((16, DK), BF16),
        in_specs=[vmem] * 3 + [hbm] * 6,
        out_specs=vmem,
        scratch_shapes=[
            pltpu.VMEM((E, 2 * FH, DK), BF16),
            pltpu.VMEM((E, 256, DK), BF16),
            pltpu.VMEM((3, E, 8, FH), F32),
            pltpu.VMEM((FH, 128), F32),
            pltpu.VMEM((FH, 128), F32),
            pltpu.VMEM((8, 128), F32),
            pltpu.VMEM((8, 2, 4, 16, DK), BF16),
            pltpu.VMEM((8, 2, 4, 1, 128), F32),
            pltpu.VMEM((DK, 256), BF16),
            pltpu.VMEM((4, 2, 2, 2 * FH, 128), F32),
            pltpu.VMEM((4, 2, 8, 128), F32),
            pltpu.VMEM((4, 2, 2 * FH, 128), BF16),
            pltpu.VMEM((4, 2, 2 * FH, 128), BF16),
            pltpu.VMEM((4, 2 * FH, 128), BF16),
            pltpu.VMEM((4, 2 * FH, 128), BF16),
            pltpu.VMEM((4, 2, 2, FH, 128), BF16),
            pltpu.VMEM((256, E * 256), BF16),
            pltpu.VMEM((2, 8, 2, 4, 16, HW), BF16),
            pltpu.VMEM((2, 8, 2, 2, 16, HW), BF16),
            pltpu.VMEM((2, 8, 2, 16, HW), BF16),
            pltpu.VMEM((2, 8, 2, 16, HW), BF16),
            pltpu.VMEM((8, 2, 2, 16, HW), BF16),
            pltpu.VMEM((16, 2, 16, HW), BF16),
            sems((6,)),
            sems((8,)),
            sems((3, 8)),
            sems((3, 8)),
            sems((4, 4)),
            sems((3, 4)),
            sems,
        ],
        compiler_params=pltpu.CompilerParams(
            collective_id=0, has_side_effects=True, vmem_limit_bytes=60 * 1024 * 1024
        ),
        name="expert_step",
    )(
        tokens, logits.T, ids.T, gate_codes, jnp.swapaxes(gate_scales, 1, 2),
        up_codes, jnp.swapaxes(up_scales, 1, 2), down_codes, jnp.swapaxes(down_scales, 1, 2),
    )


def solution(mesh):
    wide = P(None, "fsdp", "tp")
    in_specs = (P("fsdp", "tp"), P("fsdp", None), P("fsdp", None)) + (wide,) * 6
    return jax.shard_map(body, mesh=mesh, in_specs=in_specs, out_specs=P("fsdp", "tp"), check_vma=False)
```

```python
import jax
import jax.numpy as jnp
from jax import lax
from jax.experimental import pallas as pl
from jax.experimental.pallas import tpu as pltpu
from jax.sharding import PartitionSpec as P

F32, BF16 = jnp.float32, jnp.bfloat16
MESH = pl.DeviceIdType.MESH
E, FH, DK = 8, 224, 1024
GROUP = 4
HW = DK // 2
OFFSETS = (2, -2, 3, -3, 4, -1, 1, 0)


def pos_of(r):
    return OFFSETS.index(r)


def kernel(
    tok_ref, log_ref, ids_ref, gc_ref, gs_ref, uc_ref, us_ref, dc_ref, ds_ref,
    out_ref,
    wgu, dw, sc, tgu, td, flip, xbuf, rbuf, xt, acc, rt, pb, rb, yb, yr, hb, am, part, r1, s2, r2, zs, rz,
    w_sem, out_sem, g_recv, h_recv, t_recv, x_recv, z_recv,
):
    f, t = lax.axis_index("fsdp"), lax.axis_index("tp")
    z, blk = f // 8, f % 8
    y, x = blk // 4, blk % 4
    yh, core = t // 2, t % 2
    xa = x + 1 - 2 * (x % 2)
    xb = 3 - x
    xd = 3 - xa
    left, right, far = (x + 3) % 4, (x + 1) % 4, (x + 2) % 4
    own = pos_of(0)
    nought = f // 64

    def fid(zz, yy, xx):
        return (zz * 2 + yy) * 4 + xx

    def dev(ff, tt):
        return {"fsdp": ff, "tp": tt}

    def zoff(r):
        return (z + r + 8) % 8

    sibling = dev(f, yh * 2 + 1 - core)
    partner = dev(f, (1 - yh) * 2 + core)

    def copy(src, dst, ssem, rsem, to):
        return pltpu.make_async_remote_copy(
            src_ref=src, dst_ref=dst, send_sem=ssem, recv_sem=rsem, device_id=to, device_id_type=MESH
        )

    G, H, PB, YB, HB, X1, X2, Z = range(8)

    def send(src, dst, kind, rsem, to):
        copy(src, dst, out_sem.at[kind], rsem, to).start()

    def arrived(dst, rsem):
        copy(dst, dst, out_sem.at[G], rsem, sibling).wait_recv()

    def all_sent(src, kind):
        copy(src, src, out_sem.at[kind], out_sem.at[kind], sibling).wait_send()

    barrier = pltpu.get_barrier_semaphore()
    friends = [dev(fid(zoff(r), (y + dy) % 2, x), t) for r in OFFSETS for dy in (0, 1) if r or dy]
    friends += [dev(fid(z, y, left), t), dev(fid(z, y, right), t), sibling, partner]
    for to in friends:
        pl.semaphore_signal(barrier, inc=1, device_id=to, device_id_type=MESH)

    def w_copy(kind):
        src = (gc_ref, uc_ref, dc_ref)[kind]
        dst = (wgu.at[:, pl.ds(0, FH)], wgu.at[:, pl.ds(FH, FH)], dw.at[:, pl.ds(0, FH)])[kind]
        return pltpu.make_async_copy(src, dst, w_sem.at[kind])

    def s_copy(kind):
        return pltpu.make_async_copy((gs_ref, us_ref, ds_ref)[kind], sc.at[kind], w_sem.at[3 + kind])

    for kind in range(3):
        s_copy(kind).start()
    for kind in range(3):
        w_copy(kind).start()

    flip[...] = jnp.zeros((8, 128), F32)
    flip[0:2, 0:16] = ids_ref[...].astype(F32)
    flip[2:4, 0:16] = log_ref[...].astype(F32)
    xbuf[own, y, x] = tok_ref[...]
    rbuf[own, y, x] = jnp.sum(pltpu.roll(flip[...], 0, 1, stride=16, stride_axis=0), axis=0, keepdims=True)

    def enter():
        pl.semaphore_wait(barrier, len(friends))

    def both(src, dst, kind, at, to, routes=True):
        send(xbuf.at[src], xbuf.at[dst], G, g_recv.at[kind, at], to)
        if routes:
            send(rbuf.at[src[:3]], rbuf.at[dst[:3]], H, h_recv.at[kind, at], to)

    every = slice(None)
    low, high = slice(0, HW), slice(HW, DK)

    def spread():
        for to in (right, left):
            both((own, y, x), (own, y, x), 1, own, dev(fid(z, y, to), t))
        for at, r in enumerate(OFFSETS):
            for dy in (0, 1):
                if r or dy:
                    both((own, y, x), (at, y, x), 0, at, dev(fid(zoff(-r), (y + dy) % 2, x), t))

    def along_x(at):
        rows = every if OFFSETS[at] else 1 - y
        arrived(xbuf.at[at, rows, x], g_recv.at[0, at])
        arrived(rbuf.at[at, rows, x], h_recv.at[0, at])
        for to in (right, left):
            both((at, rows, x), (at, rows, x), 1, at, dev(fid(z, y, to), t))

    def along_x_again(at):
        arrived(xbuf.at[at, 0], g_recv.at[1, at])
        arrived(rbuf.at[at, 0], h_recv.at[1, at])
        here = (at, every, left, every, low)
        both(here, here, 2, at, dev(fid(z, y, right), t))
        here = (at, every, right, every, high)
        both(here, here, 2, at, dev(fid(z, y, left), t), False)

    def plane_complete(at):
        arrived(xbuf.at[at, every, far], g_recv.at[2, at])
        arrived(rbuf.at[at, every, far], h_recv.at[2, at])

    lanes = lax.broadcasted_iota(jnp.int32, (8, 128), 1) // 16
    on_row = lanes == lax.broadcasted_iota(jnp.int32, (8, 128), 0)

    def unpack_routes(at):
        rows = jnp.concatenate([rbuf[at, i // 4, i % 4] for i in range(8)], axis=0)
        rows = pltpu.roll(rows, 0, 1, stride=16, stride_axis=0)
        for v in range(4):
            turned = pltpu.roll(rows, 128 - 16 * v, 1) if v else rows
            rt[at // 2, at % 2, v : v + 1, :] = jnp.sum(jnp.where(on_row, turned, 0.0), axis=0, keepdims=True)

    def turn_scales():
        for kind in range(3):
            s_copy(kind).wait()
        for kinds, dst in ((slice(0, 2), tgu), (slice(2, 3), td)):
            rows = sc[kinds].reshape(-1, FH)
            if rows.shape[0] < 128:
                rows = jnp.concatenate([rows, jnp.zeros((128 - rows.shape[0], FH), F32)], axis=0)
            dst[0:128] = rows[:, 0:128].T
            dst[128:FH] = jnp.concatenate([rows[:, 128:FH], jnp.zeros((128, 256 - FH), F32)], axis=1).T[0 : FH - 128]
        for kind in range(3):
            w_copy(kind).wait()

    def scale_gate_up(lo, hi):
        @pl.loop(lo, hi)
        def _(e):
            scales = pltpu.roll(tgu[...], (128 - 8 * e) % 128, 1)
            for at, lane in ((0, 0), (FH, 64)):
                for b in range(8):
                    cols = slice(b * 128, (b + 1) * 128)
                    w = wgu[e, at : at + FH, cols].astype(F32) * scales[:, lane + b : lane + b + 1]
                    wgu[e, at : at + FH, cols] = w.astype(BF16)

    def scale_down(lo, hi):
        @pl.loop(lo, hi)
        def _(e):
            dw[e, FH:256, :] = jnp.zeros((256 - FH, DK), BF16)
            scales = pltpu.roll(td[...], (128 - 8 * e) % 128, 1)
            for b in range(8):
                cols = slice(b * 128, (b + 1) * 128)
                w = dw[e, 0:FH, cols].astype(F32) * scales[:, b : b + 1]
                dw[e, 0:FH, cols] = w.astype(BF16)

    def gate_up(c, g):
        if g == 0:
            for hh in (0, 1):
                plane_complete(2 * c + hh)
                unpack_routes(2 * c + hh)
            xt[...] = xbuf[2 * c : 2 * c + 2].reshape(256, DK).T

        @pl.loop(g + nought, g + 1 + nought)
        def _(g):
            w = wgu[pl.ds(g * GROUP, GROUP)].reshape(GROUP * 2 * FH, DK)
            o = jnp.dot(w, xt[...], preferred_element_type=F32)
            for i in range(GROUP):
                e = jnp.asarray(g * GROUP + i, jnp.int32).astype(F32)
                for k in (0, 1):
                    for hh in (0, 1):
                        mine = o[i * 2 * FH : (i + 1) * 2 * FH, hh * 128 : (hh + 1) * 128]
                        acc[c, k, hh] = jnp.where(rt[c, hh, k : k + 1, :] == e, mine, acc[c, k, hh])

        if g == E // GROUP - 1:
            pb[c] = acc[c, 1 - core].astype(BF16)
            send(pb.at[c], rb.at[c], PB, t_recv.at[0, c], sibling)

    def pair_sum(c, hh):
        return acc[c, core, hh] + rb[c, hh].astype(F32)

    def core_sum(c):
        arrived(rb.at[c], t_recv.at[0, c])
        for hh in (0, 1):
            yb[c, hh] = pair_sum(c, hh).astype(BF16)
        send(yb.at[c], yr.at[c], YB, t_recv.at[1, c], partner)

    def activate(c):
        arrived(yr.at[c], t_recv.at[1, c])
        for hh in (0, 1):
            total = pair_sum(c, hh) + yr[c, hh].astype(F32)
            gate, up = total[0:FH], total[FH : 2 * FH]
            route = rt[c, hh]
            diff = route[3:4] - route[2:3]
            w = 1.0 / (1.0 + jnp.exp(jnp.where(core == 0, diff, -diff)))
            hb[c, core, hh] = (gate / (1.0 + jnp.exp(-gate)) * up * w).astype(BF16)
        send(hb.at[c, core], hb.at[c, core], HB, t_recv.at[2, c], sibling)

    def down(c):
        arrived(hb.at[c, 1 - core], t_recv.at[2, c])
        pad = jnp.zeros((256 - FH, 128), F32)
        for hh in (0, 1):
            here = slice(hh * 128, (hh + 1) * 128)
            route = rt[c, hh].T
            units = [jnp.concatenate([hb[c, k, hh].astype(F32), pad], axis=0).T for k in (0, 1)]
            for e in range(E):
                both = jnp.where(route[:, 0:1] == float(e), units[0], 0.0)
                both = jnp.where(route[:, 1:2] == float(e), units[1], both)
                am[here, e * 256 : (e + 1) * 256] = both.astype(BF16)
        two = pl.ds(2 * c, 2)
        for j in range(4):
            w = dw[:, :, j * 256 : (j + 1) * 256].reshape(E * 256, 256)
            o = jnp.dot(am[...], w, preferred_element_type=F32)
            half, at = j // 2, (j % 2) * 256
            part[half, 2 * c : 2 * c + 2, :, :, :, at : at + 256] = o.astype(BF16).reshape(2, 2, 4, 16, 256)
            if j % 2:
                to = dev(fid(z, y, (xa, xb)[half]), t)
                send(part.at[half, two, :, xd], r1.at[half, two, :, 1], X1, x_recv.at[half, c], to)

    def x_rest(c):
        two = pl.ds(2 * c, 2)
        for half, to in ((0, xa), (1, xb)):
            send(part.at[half, two, :, to], r1.at[half, two, :, 0], X1, x_recv.at[2, c], dev(fid(z, y, to), t))

    def x_first(c):
        two = pl.ds(2 * c, 2)
        for half, second in ((0, xb), (1, xa)):
            arrived(r1.at[half, two, :, 1], x_recv.at[half, c])
            s2[half, two] = (part[half, two, :, second].astype(F32) + r1[half, two, :, 1].astype(F32)).astype(BF16)
            send(s2.at[half, two], r2.at[half, two], X2, x_recv.at[3, c], dev(fid(z, y, second), t))

    def x_second(c):
        two = pl.ds(2 * c, 2)
        arrived(r1.at[:, two, :, 0], x_recv.at[2, c])
        arrived(r2.at[:, two], x_recv.at[3, c])
        for half in (0, 1):
            total = part[half, two, :, x].astype(F32) + r1[half, two, :, 0].astype(F32) + r2[half, two].astype(F32)
            zs[two, :, half] = total.astype(BF16)
        for at in (2 * c, 2 * c + 1):
            for dy in (0, 1):
                if OFFSETS[at] or dy:
                    yy = (y + dy) % 2
                    to = dev(fid(zoff(OFFSETS[at]), yy, x), t)
                    send(zs.at[at, yy], rz.at[2 * at + dy], Z, z_recv, to)

    def finish():
        arrived(rz.at[pl.ds(0, 15)], z_recv)
        total = zs[own, y].astype(F32)
        for i in range(16):
            if i != 2 * own:
                total = total + rz[i].astype(F32)
        for half in (0, 1):
            out_ref[:, half * HW : (half + 1) * HW] = total[half].astype(BF16)

    def leave():
        all_sent(xbuf.reshape(64, 16, DK).at[pl.ds(0, 63)], G)
        all_sent(rbuf.reshape(64, 1, 128).at[pl.ds(0, 63)], H)
        all_sent(pb, PB)
        all_sent(yb, YB)
        all_sent(hb.at[pl.ds(0, 2)], HB)
        all_sent(r1, X1)
        all_sent(s2, X2)
        all_sent(rz.at[pl.ds(0, 15)], Z)

    schedule = (
        (enter,),
        (spread,),
        (turn_scales,),
        (scale_gate_up, 0, 6),
        (along_x, 0), (along_x, 1),
        (scale_gate_up, 6, 8),
        (along_x, 7),
        (scale_down, 0, 2),
        (along_x, 2),
        (scale_down, 2, 3),
        (along_x, 3),
        (along_x_again, 0), (along_x_again, 1),
        (along_x, 4),
        (scale_down, 3, 6),
        (along_x, 5),
        (along_x_again, 2), (along_x_again, 3),
        (along_x, 6),
        (gate_up, 0, 0),
        (along_x_again, 7), (along_x_again, 4),
        (gate_up, 0, 1),
        (along_x_again, 5),
        (scale_down, 6, 8),
        (core_sum, 0),
        (gate_up, 1, 0),
        (along_x_again, 6),
        (gate_up, 1, 1),
        (gate_up, 2, 0),
        (core_sum, 1),
        (gate_up, 2, 1),
        (gate_up, 3, 0),
        (core_sum, 2),
        (gate_up, 3, 1),
        (activate, 0),
        (core_sum, 3),
        (down, 0), (x_rest, 0),
        (activate, 1),
        (down, 1), (x_rest, 1),
        (x_first, 0),
        (activate, 2),
        (down, 2), (x_rest, 2),
        (x_first, 1),
        (x_second, 0),
        (activate, 3),
        (x_first, 2),
        (down, 3), (x_rest, 3),
        (x_second, 1),
        (x_second, 2),
        (x_first, 3),
        (x_second, 3),
        (finish,),
        (leave,),
    )
    for step, *args in schedule:
        with jax.named_scope("_".join([step.__name__, *map(str, args)])):
            step(*args)


def body(tokens, logits, ids, gate_codes, gate_scales, up_codes, up_scales, down_codes, down_scales):
    vmem = pl.BlockSpec(memory_space=pltpu.VMEM)
    hbm = pl.BlockSpec(memory_space=pl.ANY)
    sems = pltpu.SemaphoreType.DMA
    return pl.pallas_call(
        kernel,
        out_shape=jax.ShapeDtypeStruct((16, DK), BF16),
        in_specs=[vmem] * 3 + [hbm] * 6,
        out_specs=vmem,
        scratch_shapes=[
            pltpu.VMEM((E, 2 * FH, DK), BF16),
            pltpu.VMEM((E, 256, DK), BF16),
            pltpu.VMEM((3, E, 8, FH), F32),
            pltpu.VMEM((FH, 128), F32),
            pltpu.VMEM((FH, 128), F32),
            pltpu.VMEM((8, 128), F32),
            pltpu.VMEM((8, 2, 4, 16, DK), BF16),
            pltpu.VMEM((8, 2, 4, 1, 128), F32),
            pltpu.VMEM((DK, 256), BF16),
            pltpu.VMEM((4, 2, 2, 2 * FH, 128), F32),
            pltpu.VMEM((4, 2, 8, 128), F32),
            pltpu.VMEM((4, 2, 2 * FH, 128), BF16),
            pltpu.VMEM((4, 2, 2 * FH, 128), BF16),
            pltpu.VMEM((4, 2, 2 * FH, 128), BF16),
            pltpu.VMEM((4, 2, 2 * FH, 128), BF16),
            pltpu.VMEM((4, 2, 2, FH, 128), BF16),
            pltpu.VMEM((256, E * 256), BF16),
            pltpu.VMEM((2, 8, 2, 4, 16, HW), BF16),
            pltpu.VMEM((2, 8, 2, 2, 16, HW), BF16),
            pltpu.VMEM((2, 8, 2, 16, HW), BF16),
            pltpu.VMEM((2, 8, 2, 16, HW), BF16),
            pltpu.VMEM((8, 2, 2, 16, HW), BF16),
            pltpu.VMEM((16, 2, 16, HW), BF16),
            sems((6,)),
            sems((8,)),
            sems((3, 8)),
            sems((3, 8)),
            sems((3, 4)),
            sems((4, 4)),
            sems,
        ],
        compiler_params=pltpu.CompilerParams(
            collective_id=0, has_side_effects=True, vmem_limit_bytes=60 * 1024 * 1024
        ),
        name="expert_step",
    )(
        tokens, logits.T, ids.T, gate_codes, jnp.swapaxes(gate_scales, 1, 2),
        up_codes, jnp.swapaxes(up_scales, 1, 2), down_codes, jnp.swapaxes(down_scales, 1, 2),
    )


def solution(mesh):
    wide = P(None, "fsdp", "tp")
    in_specs = (P("fsdp", "tp"), P("fsdp", None), P("fsdp", None)) + (wide,) * 6
    return jax.shard_map(body, mesh=mesh, in_specs=in_specs, out_specs=P("fsdp", "tp"), check_vma=False)
```

```python
import jax
import jax.numpy as jnp
from jax import lax
from jax.experimental import pallas as pl
from jax.experimental.pallas import tpu as pltpu
from jax.sharding import PartitionSpec as P

F32, BF16 = jnp.float32, jnp.bfloat16
MESH = pl.DeviceIdType.MESH
E, FH, DK = 8, 224, 1024
GROUP = 4
HW = DK // 2
OFFSETS = (2, -2, 3, -3, 4, -1, 1, 0)
DIRECT = (0, 1)


def pos_of(r):
    return OFFSETS.index(r)


def kernel(
    tok_ref, log_ref, ids_ref, gc_ref, gs_ref, uc_ref, us_ref, dc_ref, ds_ref,
    out_ref,
    wgu, dw, sc, tgu, td, flip, xbuf, rbuf, xt, acc, rt, pb, rb, yb, yr, hb, am, part, r1, s2, r2, zs, rz,
    w_sem, out_sem, g_recv, h_recv, t_recv, x_recv, z_recv,
):
    f, t = lax.axis_index("fsdp"), lax.axis_index("tp")
    z, blk = f // 8, f % 8
    y, x = blk // 4, blk % 4
    yh, core = t // 2, t % 2
    xa = x + 1 - 2 * (x % 2)
    xb = 3 - x
    xd = 3 - xa
    left, right, far = (x + 3) % 4, (x + 1) % 4, (x + 2) % 4
    own = pos_of(0)
    nought = f // 64

    def fid(zz, yy, xx):
        return (zz * 2 + yy) * 4 + xx

    def dev(ff, tt):
        return {"fsdp": ff, "tp": tt}

    def zoff(r):
        return (z + r + 8) % 8

    sibling = dev(f, yh * 2 + 1 - core)
    partner = dev(f, (1 - yh) * 2 + core)

    def copy(src, dst, ssem, rsem, to):
        return pltpu.make_async_remote_copy(
            src_ref=src, dst_ref=dst, send_sem=ssem, recv_sem=rsem, device_id=to, device_id_type=MESH
        )

    G, H, PB, YB, HB, X1, X2, Z = range(8)

    def send(src, dst, kind, rsem, to):
        copy(src, dst, out_sem.at[kind], rsem, to).start()

    def arrived(dst, rsem):
        copy(dst, dst, out_sem.at[G], rsem, sibling).wait_recv()

    def all_sent(src, kind):
        copy(src, src, out_sem.at[kind], out_sem.at[kind], sibling).wait_send()

    barrier = pltpu.get_barrier_semaphore()
    friends = [dev(fid(zoff(r), (y + dy) % 2, x), t) for r in OFFSETS for dy in (0, 1) if r or dy]
    friends += [dev(fid(z, y, xx), t) for xx in (left, right, far)] + [sibling, partner]
    for to in friends:
        pl.semaphore_signal(barrier, inc=1, device_id=to, device_id_type=MESH)

    def w_copy(kind):
        src = (gc_ref, uc_ref, dc_ref)[kind]
        dst = (wgu.at[:, pl.ds(0, FH)], wgu.at[:, pl.ds(FH, FH)], dw.at[:, pl.ds(0, FH)])[kind]
        return pltpu.make_async_copy(src, dst, w_sem.at[kind])

    def s_copy(kind):
        return pltpu.make_async_copy((gs_ref, us_ref, ds_ref)[kind], sc.at[kind], w_sem.at[3 + kind])

    for kind in range(3):
        s_copy(kind).start()
    for kind in range(3):
        w_copy(kind).start()

    flip[...] = jnp.zeros((8, 128), F32)
    flip[0:2, 0:16] = ids_ref[...].astype(F32)
    flip[2:4, 0:16] = log_ref[...].astype(F32)
    xbuf[own, y, x] = tok_ref[...]
    rbuf[own, y, x] = jnp.sum(pltpu.roll(flip[...], 0, 1, stride=16, stride_axis=0), axis=0, keepdims=True)

    def enter():
        pl.semaphore_wait(barrier, len(friends))

    def both(src, dst, kind, at, to, routes=True):
        send(xbuf.at[src], xbuf.at[dst], G, g_recv.at[kind, at], to)
        if routes:
            send(rbuf.at[src[:3]], rbuf.at[dst[:3]], H, h_recv.at[kind, at], to)

    every = slice(None)
    low, high = slice(0, HW), slice(HW, DK)

    def spread():
        for to in (right, left):
            both((own, y, x), (own, y, x), 1, own, dev(fid(z, y, to), t))
        for at, r in enumerate(OFFSETS):
            for dy in (0, 1):
                if r or dy:
                    both((own, y, x), (at, y, x), 0, at, dev(fid(zoff(-r), (y + dy) % 2, x), t))

    def along_x(at):
        rows = every if OFFSETS[at] else 1 - y
        arrived(xbuf.at[at, rows, x], g_recv.at[0, at])
        arrived(rbuf.at[at, rows, x], h_recv.at[0, at])
        for to in (right, left):
            both((at, rows, x), (at, rows, x), 1, at, dev(fid(z, y, to), t))
        if at in DIRECT:
            both((at, every, x), (at, every, x), 2, at, dev(fid(z, y, far), t))

    def along_x_again(at):
        arrived(xbuf.at[at, 0], g_recv.at[1, at])
        arrived(rbuf.at[at, 0], h_recv.at[1, at])
        if at in DIRECT:
            return
        here = (at, every, left, every, low)
        both(here, here, 2, at, dev(fid(z, y, right), t))
        here = (at, every, right, every, high)
        both(here, here, 2, at, dev(fid(z, y, left), t), False)

    def plane_complete(at):
        arrived(xbuf.at[at, every, far], g_recv.at[2, at])
        arrived(rbuf.at[at, every, far], h_recv.at[2, at])

    lanes = lax.broadcasted_iota(jnp.int32, (8, 128), 1) // 16
    on_row = lanes == lax.broadcasted_iota(jnp.int32, (8, 128), 0)

    def unpack_routes(at):
        rows = jnp.concatenate([rbuf[at, i // 4, i % 4] for i in range(8)], axis=0)
        rows = pltpu.roll(rows, 0, 1, stride=16, stride_axis=0)
        for v in range(4):
            turned = pltpu.roll(rows, 128 - 16 * v, 1) if v else rows
            rt[at // 2, at % 2, v : v + 1, :] = jnp.sum(jnp.where(on_row, turned, 0.0), axis=0, keepdims=True)

    def turn_scales():
        for kind in range(3):
            s_copy(kind).wait()
        for kinds, dst in ((slice(0, 2), tgu), (slice(2, 3), td)):
            rows = sc[kinds].reshape(-1, FH)
            if rows.shape[0] < 128:
                rows = jnp.concatenate([rows, jnp.zeros((128 - rows.shape[0], FH), F32)], axis=0)
            dst[0:128] = rows[:, 0:128].T
            dst[128:FH] = jnp.concatenate([rows[:, 128:FH], jnp.zeros((128, 256 - FH), F32)], axis=1).T[0 : FH - 128]
        for kind in range(3):
            w_copy(kind).wait()

    def scale_gate_up(lo, hi):
        @pl.loop(lo, hi)
        def _(e):
            scales = pltpu.roll(tgu[...], (128 - 8 * e) % 128, 1)
            for at, lane in ((0, 0), (FH, 64)):
                for b in range(8):
                    cols = slice(b * 128, (b + 1) * 128)
                    w = wgu[e, at : at + FH, cols].astype(F32) * scales[:, lane + b : lane + b + 1]
                    wgu[e, at : at + FH, cols] = w.astype(BF16)

    def scale_down(lo, hi):
        @pl.loop(lo, hi)
        def _(e):
            dw[e, FH:256, :] = jnp.zeros((256 - FH, DK), BF16)
            scales = pltpu.roll(td[...], (128 - 8 * e) % 128, 1)
            for b in range(8):
                cols = slice(b * 128, (b + 1) * 128)
                w = dw[e, 0:FH, cols].astype(F32) * scales[:, b : b + 1]
                dw[e, 0:FH, cols] = w.astype(BF16)

    def gate_up(c, g):
        if g == 0:
            for hh in (0, 1):
                plane_complete(2 * c + hh)
                unpack_routes(2 * c + hh)
            xt[...] = xbuf[2 * c : 2 * c + 2].reshape(256, DK).T

        @pl.loop(g + nought, g + 1 + nought)
        def _(g):
            w = wgu[pl.ds(g * GROUP, GROUP)].reshape(GROUP * 2 * FH, DK)
            o = jnp.dot(w, xt[...], preferred_element_type=F32)
            for i in range(GROUP):
                e = jnp.asarray(g * GROUP + i, jnp.int32).astype(F32)
                for k in (0, 1):
                    for hh in (0, 1):
                        mine = o[i * 2 * FH : (i + 1) * 2 * FH, hh * 128 : (hh + 1) * 128]
                        acc[c, k, hh] = jnp.where(rt[c, hh, k : k + 1, :] == e, mine, acc[c, k, hh])

        if g == E // GROUP - 1:
            pb[c] = acc[c, 1 - core].astype(BF16)
            send(pb.at[c], rb.at[c], PB, t_recv.at[0, c], sibling)

    def pair_sum(c, hh):
        return acc[c, core, hh] + rb[c, hh].astype(F32)

    def core_sum(c):
        arrived(rb.at[c], t_recv.at[0, c])
        for hh in (0, 1):
            yb[c, hh] = pair_sum(c, hh).astype(BF16)
        send(yb.at[c], yr.at[c], YB, t_recv.at[1, c], partner)

    def activate(c):
        arrived(yr.at[c], t_recv.at[1, c])
        for hh in (0, 1):
            total = pair_sum(c, hh) + yr[c, hh].astype(F32)
            gate, up = total[0:FH], total[FH : 2 * FH]
            route = rt[c, hh]
            diff = route[3:4] - route[2:3]
            w = 1.0 / (1.0 + jnp.exp(jnp.where(core == 0, diff, -diff)))
            hb[c, core, hh] = (gate / (1.0 + jnp.exp(-gate)) * up * w).astype(BF16)
        send(hb.at[c, core], hb.at[c, core], HB, t_recv.at[2, c], sibling)

    def down(c):
        arrived(hb.at[c, 1 - core], t_recv.at[2, c])
        pad = jnp.zeros((256 - FH, 128), F32)
        for hh in (0, 1):
            here = slice(hh * 128, (hh + 1) * 128)
            route = rt[c, hh].T
            units = [jnp.concatenate([hb[c, k, hh].astype(F32), pad], axis=0).T for k in (0, 1)]
            for e in range(E):
                both = jnp.where(route[:, 0:1] == float(e), units[0], 0.0)
                both = jnp.where(route[:, 1:2] == float(e), units[1], both)
                am[here, e * 256 : (e + 1) * 256] = both.astype(BF16)
        two = pl.ds(2 * c, 2)
        for j in range(4):
            w = dw[:, :, j * 256 : (j + 1) * 256].reshape(E * 256, 256)
            o = jnp.dot(am[...], w, preferred_element_type=F32)
            half, at = j // 2, (j % 2) * 256
            part[half, 2 * c : 2 * c + 2, :, :, :, at : at + 256] = o.astype(BF16).reshape(2, 2, 4, 16, 256)
            if j % 2:
                to = dev(fid(z, y, (xa, xb)[half]), t)
                send(part.at[half, two, :, xd], r1.at[half, two, :, 1], X1, x_recv.at[half, c], to)

    def x_rest(c):
        two = pl.ds(2 * c, 2)
        for half, to in ((0, xa), (1, xb)):
            send(part.at[half, two, :, to], r1.at[half, two, :, 0], X1, x_recv.at[2, c], dev(fid(z, y, to), t))

    def x_first(c):
        two = pl.ds(2 * c, 2)
        for half, second in ((0, xb), (1, xa)):
            arrived(r1.at[half, two, :, 1], x_recv.at[half, c])
            s2[half, two] = (part[half, two, :, second].astype(F32) + r1[half, two, :, 1].astype(F32)).astype(BF16)
            send(s2.at[half, two], r2.at[half, two], X2, x_recv.at[3, c], dev(fid(z, y, second), t))

    def x_second(c):
        two = pl.ds(2 * c, 2)
        arrived(r1.at[:, two, :, 0], x_recv.at[2, c])
        arrived(r2.at[:, two], x_recv.at[3, c])
        for half in (0, 1):
            total = part[half, two, :, x].astype(F32) + r1[half, two, :, 0].astype(F32) + r2[half, two].astype(F32)
            zs[two, :, half] = total.astype(BF16)
        for at in (2 * c, 2 * c + 1):
            for dy in (0, 1):
                if OFFSETS[at] or dy:
                    yy = (y + dy) % 2
                    to = dev(fid(zoff(OFFSETS[at]), yy, x), t)
                    send(zs.at[at, yy], rz.at[2 * at + dy], Z, z_recv, to)

    def finish():
        arrived(rz.at[pl.ds(0, 15)], z_recv)
        total = zs[own, y].astype(F32)
        for i in range(16):
            if i != 2 * own:
                total = total + rz[i].astype(F32)
        for half in (0, 1):
            out_ref[:, half * HW : (half + 1) * HW] = total[half].astype(BF16)

    def leave():
        all_sent(xbuf.reshape(64, 16, DK).at[pl.ds(0, 63)], G)
        all_sent(rbuf.reshape(64, 1, 128).at[pl.ds(0, 63)], H)
        all_sent(pb, PB)
        all_sent(yb, YB)
        all_sent(hb.at[pl.ds(0, 2)], HB)
        all_sent(r1, X1)
        all_sent(s2, X2)
        all_sent(rz.at[pl.ds(0, 15)], Z)

    schedule = (
        (enter,),
        (spread,),
        (turn_scales,),
        (scale_gate_up, 0, 6),
        (along_x, 0), (along_x, 1),
        (scale_gate_up, 6, 8),
        (along_x, 7),
        (scale_down, 0, 2),
        (along_x, 2),
        (scale_down, 2, 3),
        (along_x, 3),
        (along_x, 4),
        (scale_down, 3, 6),
        (along_x, 5),
        (along_x, 6),
        (along_x_again, 0), (along_x_again, 1),
        (gate_up, 0, 0),
        (along_x_again, 2), (along_x_again, 3), (along_x_again, 7),
        (gate_up, 0, 1),
        (along_x_again, 4),
        (along_x_again, 5),
        (scale_down, 6, 8),
        (core_sum, 0),
        (gate_up, 1, 0),
        (along_x_again, 6),
        (gate_up, 1, 1),
        (gate_up, 2, 0),
        (core_sum, 1),
        (gate_up, 2, 1),
        (gate_up, 3, 0),
        (core_sum, 2),
        (gate_up, 3, 1),
        (activate, 0),
        (core_sum, 3),
        (down, 0), (x_rest, 0),
        (activate, 1),
        (down, 1), (x_rest, 1),
        (x_first, 0),
        (activate, 2),
        (down, 2), (x_rest, 2),
        (x_first, 1),
        (x_second, 0),
        (activate, 3),
        (x_first, 2),
        (down, 3), (x_rest, 3),
        (x_second, 1),
        (x_second, 2),
        (x_first, 3),
        (x_second, 3),
        (finish,),
        (leave,),
    )
    for step, *args in schedule:
        with jax.named_scope("_".join([step.__name__, *map(str, args)])):
            step(*args)


def body(tokens, logits, ids, gate_codes, gate_scales, up_codes, up_scales, down_codes, down_scales):
    vmem = pl.BlockSpec(memory_space=pltpu.VMEM)
    hbm = pl.BlockSpec(memory_space=pl.ANY)
    sems = pltpu.SemaphoreType.DMA
    return pl.pallas_call(
        kernel,
        out_shape=jax.ShapeDtypeStruct((16, DK), BF16),
        in_specs=[vmem] * 3 + [hbm] * 6,
        out_specs=vmem,
        scratch_shapes=[
            pltpu.VMEM((E, 2 * FH, DK), BF16),
            pltpu.VMEM((E, 256, DK), BF16),
            pltpu.VMEM((3, E, 8, FH), F32),
            pltpu.VMEM((FH, 128), F32),
            pltpu.VMEM((FH, 128), F32),
            pltpu.VMEM((8, 128), F32),
            pltpu.VMEM((8, 2, 4, 16, DK), BF16),
            pltpu.VMEM((8, 2, 4, 1, 128), F32),
            pltpu.VMEM((DK, 256), BF16),
            pltpu.VMEM((4, 2, 2, 2 * FH, 128), F32),
            pltpu.VMEM((4, 2, 8, 128), F32),
            pltpu.VMEM((4, 2, 2 * FH, 128), BF16),
            pltpu.VMEM((4, 2, 2 * FH, 128), BF16),
            pltpu.VMEM((4, 2, 2 * FH, 128), BF16),
            pltpu.VMEM((4, 2, 2 * FH, 128), BF16),
            pltpu.VMEM((4, 2, 2, FH, 128), BF16),
            pltpu.VMEM((256, E * 256), BF16),
            pltpu.VMEM((2, 8, 2, 4, 16, HW), BF16),
            pltpu.VMEM((2, 8, 2, 2, 16, HW), BF16),
            pltpu.VMEM((2, 8, 2, 16, HW), BF16),
            pltpu.VMEM((2, 8, 2, 16, HW), BF16),
            pltpu.VMEM((8, 2, 2, 16, HW), BF16),
            pltpu.VMEM((16, 2, 16, HW), BF16),
            sems((6,)),
            sems((8,)),
            sems((3, 8)),
            sems((3, 8)),
            sems((3, 4)),
            sems((4, 4)),
            sems,
        ],
        compiler_params=pltpu.CompilerParams(
            collective_id=0, has_side_effects=True, vmem_limit_bytes=60 * 1024 * 1024
        ),
        name="expert_step",
    )(
        tokens, logits.T, ids.T, gate_codes, jnp.swapaxes(gate_scales, 1, 2),
        up_codes, jnp.swapaxes(up_scales, 1, 2), down_codes, jnp.swapaxes(down_scales, 1, 2),
    )


def solution(mesh):
    wide = P(None, "fsdp", "tp")
    in_specs = (P("fsdp", "tp"), P("fsdp", None), P("fsdp", None)) + (wide,) * 6
    return jax.shard_map(body, mesh=mesh, in_specs=in_specs, out_specs=P("fsdp", "tp"), check_vma=False)
```
